128 devices in a mesh: north: 32 (over z, x, core), deep: 4 (over y).
Axes of the slice: x: 4, y: 4, z: 4, core: 2. Of those that a mesh axis runs over, the one named last changes fastest.
Arguments:
- source: float32 [512, 512, 2048], P(None, 'north', 'deep'), may hold values from -6 to 6
- symbol_x: float32 [512], replicated, may hold values from 0.3 to 3
- symbol_y: float32 [512], replicated, may hold values from 0.3 to 3
- symbol_z: float32 [2048], replicated, may hold values from 0.3 to 3
Outputs:
- coefficients: float32 [256, 256, 1024], P('north', 'deep')
The draws below stay inside these ranges and needn't reach their ends.
All inputs are finite; a program needn't handle non-finite values.
Results may differ from the reference program's by a relative error of at most 0.000071.
Values sent between devices are 32-bit elements; how exact they have to be, the bound alone decides.
No kernel may reach another device: no remote copies, remote signals or barrier semaphores. Data moves between devices by JAX's collectives and lax.ppermute only.
A program may use at most 128 MiB of HBM per device.

```python
import jax
import jax.numpy as jnp
from jax import lax

GRID_X = 512
GRID_Y = 512
GRID_Z = 2048


def block_levels(stream_key, shape, shards, least, largest):
    gain = 1.0
    for dim, parts in shards:
        heights = jax.random.uniform(jax.random.fold_in(jax.random.fold_in(stream_key, 6), dim), (parts,), jnp.float32, least / len(shards), largest / len(shards))
        gain = gain * jnp.repeat(jnp.exp(heights), shape[dim] // parts).reshape((-1,) + (1,) * (len(shape) - 1 - dim))
    return gain


def noise(rng, shape, scale, most, shards=(), dtype=jnp.bfloat16):
    level = block_levels(rng, shape, shards, -0.22, 0.18) if shards else 1.0
    entries = jax.random.normal(rng, shape, jnp.float32) * scale * level
    return jnp.minimum(jnp.maximum(entries, -most), most).astype(dtype)


def setup_inputs(seed: int = 0) -> dict:
    arg_keys = jax.random.split(jax.random.key(seed), 5)
    source = noise(arg_keys[0], (GRID_X, GRID_Y, GRID_Z), 1.0, 6.0, ((1, 32), (2, 4)), jnp.float32)
    symbol_x = jnp.clip(jax.random.uniform(arg_keys[1], (GRID_X,), jnp.float32, 0.3, 3.0), 0.3, 3.0)
    symbol_y = jnp.clip(jax.random.uniform(arg_keys[2], (GRID_Y,), jnp.float32, 0.3, 3.0), 0.3, 3.0)
    symbol_z = jnp.clip(jax.random.uniform(arg_keys[3], (GRID_Z,), jnp.float32, 0.3, 3.0), 0.3, 3.0)
    return {"source": source, "symbol_x": symbol_x, "symbol_y": symbol_y, "symbol_z": symbol_z}


def basis_table(count):
    rank = jnp.arange(count)
    angle = jnp.pi / (count + 1) * ((rank[:, None] + 1) * (rank[None, :] + 1) % (2 * count + 2)).astype(jnp.float32)
    return jnp.sin(angle) * (2.0 / (count + 1)) ** 0.5

def along_dim(values, dim):
    moved = jnp.tensordot(values, basis_table(values.shape[dim]), axes=([dim], [0]), precision=lax.Precision.HIGHEST)
    return jnp.moveaxis(moved, -1, dim)

def reference(source, symbol_x, symbol_y, symbol_z):
    coefficients = source
    coefficients = along_dim(coefficients, 0)
    coefficients = lax.slice_in_dim(coefficients, 0, GRID_X // 2, axis=0)
    coefficients = along_dim(coefficients, 1)
    coefficients = lax.slice_in_dim(coefficients, 0, GRID_Y // 2, axis=1)
    coefficients = along_dim(coefficients, 2)
    coefficients = lax.slice_in_dim(coefficients, 0, GRID_Z // 2, axis=2)
    symbol = symbol_x[:GRID_X // 2][:, None, None] + symbol_y[:GRID_Y // 2][None, :, None] + symbol_z[:GRID_Z // 2][None, None, :]
    coefficients = coefficients * lax.rsqrt(symbol)
    return coefficients
```

```python
import jax
import jax.numpy as jnp
import numpy as np
from jax import lax
from jax.experimental import pallas as pl
from jax.experimental.pallas import tpu as pltpu
from jax.sharding import PartitionSpec as P

F32, BF16 = jnp.float32, jnp.bfloat16
NORTH, DEEP = 32, 4


def sines(rows, modes, count):
    turn = np.outer(np.asarray(rows) + 1, np.asarray(modes) + 1) % (2 * count + 2)
    return np.sin(np.pi / (count + 1) * turn) * (2.0 / (count + 1)) ** 0.5


def halves(table):
    table = np.asarray(table, np.float32)
    high = table.astype(BF16)
    return high, (table - high.astype(np.float32)).astype(BF16)


def wide(table):
    high, low = halves(table)
    return np.concatenate([high, low, high], axis=-1)


def split(values):
    high = values.astype(BF16)
    return high, (values - high.astype(F32)).astype(BF16)


def tall(values):
    high, low = split(values)
    return jnp.concatenate([high, high, low], axis=0)


def dot(a, b):
    return jnp.dot(a, b, preferred_element_type=F32)


def cost(flops, size):
    return pl.CostEstimate(flops=flops, bytes_accessed=size, transcendentals=0)


def vmem():
    return pl.BlockSpec(memory_space=pltpu.VMEM)


def x_kernel(even_ref, odd_ref, x_ref, a_ref, *refs):
    b_refs, (sums, diffs) = refs[:DEEP], refs[DEEP:]
    half = x_ref.shape[0] // 2
    me = lax.axis_index("deep")

    def fold(step, carry):
        for j in range(8):
            i = step * 8 + j
            near, far = x_ref[i], x_ref[2 * half - 1 - i]
            sums[pl.ds(pl.multiple_of(i * 8, 8), 8), :] = near + far
            diffs[pl.ds(pl.multiple_of(i * 8, 8), 8), :] = near - far
        return carry

    lax.fori_loop(0, half // 8, fold, 0)
    even = even_ref[...]
    odd = jnp.concatenate([odd_ref[me ^ k] for k in range(DEEP)], axis=0)
    a_rows = a_ref.reshape(half // 2 * 8, 128)
    b_rows = [b.reshape(NORTH * 8, 128) for b in b_refs]
    for y in range(0, 8, 2):
        s = jnp.concatenate([sums[pl.ds(y + j, half, stride=8), :] for j in range(2)], axis=1)
        e = dot(even, tall(s))
        t = jnp.concatenate([diffs[pl.ds(y + j, half, stride=8), :] for j in range(2)], axis=1)
        o = dot(odd, tall(t))
        for j in range(2):
            a_rows[pl.ds(y + j, half // 2, stride=8), :] = e[:, j * 128 : (j + 1) * 128]
            for k in range(DEEP):
                b_rows[k][pl.ds(y + j, NORTH, stride=8), :] = o[k * NORTH : (k + 1) * NORTH, j * 128 : (j + 1) * 128]


def x_stage(source):
    nx, ny, nz = source.shape
    modes = nx // 2
    block = modes // NORTH
    near = np.arange(nx // 2)
    even = wide(sines(near, np.arange(0, modes, 2), nx).T)
    odd_modes = (block * np.arange(NORTH)[None, :] + 2 * np.arange(DEEP)[:, None] + 1).reshape(-1)
    odd = wide(sines(near, odd_modes, nx).T).reshape(DEEP, NORTH, -1)
    b_shape = jax.ShapeDtypeStruct((NORTH, ny, nz), F32)
    b_spec = pl.BlockSpec((NORTH, 8, 128), lambda y, z: (0, y, z))
    return pl.pallas_call(
        x_kernel,
        grid=(ny // 8, nz // 128),
        in_specs=[vmem(), vmem(), pl.BlockSpec((nx, 8, 128), lambda y, z: (0, y, z))],
        out_specs=[pl.BlockSpec((modes // 2, 8, 128), lambda y, z: (0, y, z))] + [b_spec] * DEEP,
        out_shape=[jax.ShapeDtypeStruct((modes // 2, ny, nz), F32)] + [b_shape] * DEEP,
        scratch_shapes=[pltpu.VMEM((nx // 2 * 8, 128), F32)] * 2,
        cost_estimate=cost(6 * nx * modes * ny * nz // 2, 6 * nx * ny * nz),
        name="x_stage",
    )(jnp.asarray(even), jnp.asarray(odd), source)


def y_table(ny):
    return jnp.asarray(wide(sines(np.arange(ny), np.arange(ny // 2), ny).T).reshape(DEEP, ny // 2 // DEEP, -1))


def ya_kernel(table_ref, v_ref, *outs):
    me = lax.axis_index("deep")
    table = jnp.concatenate([table_ref[me ^ k] for k in range(DEEP)], axis=0)
    v = v_ref[...]
    n, _, y, z = v.shape
    r = dot(table, tall(v.reshape(n * y, z)))
    m = r.shape[0] // DEEP
    for k in range(DEEP):
        outs[k][0] = r[k * m : (k + 1) * m]


def ya_stage(table, v):
    n, js, y, nz = v.shape
    m = table.shape[1]
    zb = 256
    return pl.pallas_call(
        ya_kernel,
        grid=(js, nz // zb),
        in_specs=[vmem(), pl.BlockSpec((n, 1, y, zb), lambda j, z: (0, j, 0, z))],
        out_specs=[pl.BlockSpec((1, m, zb), lambda j, z: (j, 0, z))] * DEEP,
        out_shape=[jax.ShapeDtypeStruct((js, m, nz), F32)] * DEEP,
        cost_estimate=cost(6 * n * y * m * DEEP * js * nz, 6 * n * js * y * nz),
        name="ya_stage",
    )(table, v)


def z_product(table_ref, pieces, high, low):
    me = lax.axis_index("deep")

    @pl.when(pl.program_id(0) == 0)
    def _():
        for k, piece in enumerate(pieces):
            v = piece[...]
            high[k], low[k] = split(v.reshape(-1, v.shape[-1]))

    total = None
    for k in range(DEEP):
        th, tl = table_ref[me ^ k, 0], table_ref[me ^ k, 1]
        h = high[k]
        term = dot(h, th) + dot(low[k], th) + dot(h, tl)
        total = term if total is None else total + term
    return total


def zb_kernel(table_ref, p0, p1, p2, p3, o_ref, high, low):
    o_ref[...] = z_product(table_ref, (p0, p1, p2, p3), high, low).reshape(o_ref.shape)


def zb_stage(table, pieces):
    n, y, z = pieces[0].shape
    modes, block = table.shape[3], 256
    return pl.pallas_call(
        zb_kernel,
        grid=(modes // block,),
        in_specs=[pl.BlockSpec((DEEP, 2, z, block), lambda i: (0, 0, 0, i))] + [vmem()] * DEEP,
        out_specs=pl.BlockSpec((n, y, block), lambda i: (0, 0, i)),
        out_shape=jax.ShapeDtypeStruct((n, y, modes), F32),
        scratch_shapes=[pltpu.VMEM((DEEP, n * y, z), BF16)] * 2,
        cost_estimate=cost(6 * n * y * z * DEEP * modes, 4 * n * y * z * DEEP + 4 * z * DEEP * modes),
        name="zb_stage",
    )(table, *pieces)


def za_kernel(sx_ref, table_ref, sy_ref, sz_ref, p0, p1, p2, p3, o_ref, high, low):
    js, m, block = o_ref.shape[0], o_ref.shape[2], o_ref.shape[3]
    total = z_product(table_ref, (p0, p1, p2, p3), high, low)
    yz = jnp.concatenate([sy_ref[lax.axis_index("deep")]] * (block // 128), axis=1) + sz_ref[...]
    first = lax.axis_index("north") * 2 * js
    for j in range(js):
        o_ref[j, 0] = total[j * m : (j + 1) * m] * lax.rsqrt(sx_ref[first + 2 * j] + yz)


def za_stage(sx, table, sy, sz, pieces):
    js, m, z = pieces[0].shape
    modes, block = table.shape[3], 256
    return pl.pallas_call(
        za_kernel,
        grid=(modes // block,),
        in_specs=[
            pl.BlockSpec(memory_space=pltpu.SMEM),
            pl.BlockSpec((DEEP, 2, z, block), lambda i: (0, 0, 0, i)),
            vmem(),
            pl.BlockSpec((1, block), lambda i: (0, i)),
        ]
        + [vmem()] * DEEP,
        out_specs=pl.BlockSpec((js, 1, m, block), lambda i: (0, 0, 0, i)),
        out_shape=jax.ShapeDtypeStruct((js, 2, m, modes), F32),
        scratch_shapes=[pltpu.VMEM((DEEP, js * m, z), BF16)] * 2,
        cost_estimate=cost(6 * js * m * z * DEEP * modes, 4 * js * m * z * DEEP + 4 * z * DEEP * modes),
        name="za_stage",
    )(sx, table, sy, sz, *pieces)


def yb_kernel(sx_ref, table_ref, sy_ref, sz_ref, v_ref, *outs):
    me = lax.axis_index("deep")
    table = jnp.concatenate([table_ref[me ^ k] for k in range(DEEP)], axis=0)
    v = v_ref[...]
    n, y, z = v.shape
    r = dot(table, tall(v.reshape(n * y, z)))
    m = r.shape[0] // DEEP
    sx = sx_ref[lax.axis_index("north") * 2 * DEEP + 2 * me + 1]
    for k in range(DEEP):
        symbol = sx + jnp.concatenate([sy_ref[me ^ k]] * (z // 128), axis=1) + sz_ref[...]
        outs[k][...] = r[k * m : (k + 1) * m] * lax.rsqrt(symbol)


def yb_stage(sx, table, sy, sz, v):
    n, y, modes = v.shape
    m, block = table.shape[1], 256
    return pl.pallas_call(
        yb_kernel,
        grid=(modes // block,),
        in_specs=[
            pl.BlockSpec(memory_space=pltpu.SMEM),
            vmem(),
            vmem(),
            pl.BlockSpec((1, block), lambda i: (0, i)),
            pl.BlockSpec((n, y, block), lambda i: (0, 0, i)),
        ],
        out_specs=[pl.BlockSpec((m, block), lambda i: (0, i))] * DEEP,
        out_shape=[jax.ShapeDtypeStruct((m, modes), F32)] * DEEP,
        cost_estimate=cost(6 * n * y * m * DEEP * modes, 6 * n * y * modes),
        name="yb_stage",
    )(sx, table, sy, sz, v)


def join_kernel(whole_ref, p0, p1, p2, p3, o_ref, sems):
    me = lax.axis_index("deep")
    copies = [
        pltpu.make_async_copy(p, o_ref.at[me ^ k, 1], sems.at[k]) for k, p in enumerate((p0, p1, p2, p3))
    ]
    for copy in copies:
        copy.start()
    for copy in copies:
        copy.wait()


def join_stage(whole, pieces):
    return pl.pallas_call(
        join_kernel,
        in_specs=[pl.BlockSpec(memory_space=pl.ANY)] + [vmem()] * DEEP,
        out_specs=pl.BlockSpec(memory_space=pl.ANY),
        out_shape=jax.ShapeDtypeStruct(whole.shape, F32),
        scratch_shapes=[pltpu.SemaphoreType.DMA((DEEP,))],
        input_output_aliases={0: 0},
        cost_estimate=cost(1, 8 * pieces[0].size * DEEP),
        name="join_stage",
    )(whole, *pieces)


def z_table(count):
    rank = jnp.arange(count)
    turn = (rank[:, None] + 1) * (rank[None, : count // 2] + 1) % (2 * count + 2)
    table = jnp.sin(np.float32(np.pi / (count + 1)) * turn.astype(F32)) * np.float32((2.0 / (count + 1)) ** 0.5)
    high = lax.reduce_precision(table, 8, 7)
    both = jnp.stack([high, table - high]).astype(BF16)
    return both.reshape(2, DEEP, count // DEEP, count // 2).transpose(1, 0, 2, 3)


def deep_exchange(pieces):
    sent = [lax.ppermute(pieces[k], "deep", [(s, s ^ k) for s in range(DEEP)]) for k in range(1, DEEP)]
    return [pieces[0]] + sent


def north_exchange(v):
    return lax.all_to_all(v, "north", split_axis=0, concat_axis=0, tiled=True)


def on_device(source, symbol_x, symbol_y, symbol_z):
    nx, ny, nz = source.shape[0], source.shape[1] * NORTH, source.shape[2] * DEEP
    a, *b = x_stage(source)
    a = north_exchange(a.reshape(NORTH, -1, *a.shape[1:]))
    b = deep_exchange(b)
    tz = z_table(nz)
    ty = y_table(ny)
    sy = jnp.broadcast_to(symbol_y[: ny // 2, None], (ny // 2, 128)).reshape(DEEP, -1, 128)
    sz = symbol_z[None, : nz // 2]
    b = north_exchange(zb_stage(tz, b))
    a = deep_exchange(ya_stage(ty, a))
    whole = za_stage(symbol_x, tz, sy, sz, a)
    b = deep_exchange(yb_stage(symbol_x, ty, sy, sz, b))
    whole = join_stage(whole, b)
    return whole.reshape(-1, *whole.shape[2:])


def solution(mesh):
    in_specs = (P(None, "north", "deep"), P(), P(), P())
    out_specs = P("north", "deep", None)
    return jax.shard_map(
        on_device, mesh=mesh, in_specs=in_specs, out_specs=out_specs, check_vma=False
    )
```

```python
import jax
import jax.numpy as jnp
import numpy as np
from jax import lax
from jax.experimental import pallas as pl
from jax.experimental.pallas import tpu as pltpu
from jax.sharding import PartitionSpec as P

F32, BF16 = jnp.float32, jnp.bfloat16
NORTH, DEEP = 32, 4


def sines(rows, modes, count):
    turn = np.outer(np.asarray(rows) + 1, np.asarray(modes) + 1) % (2 * count + 2)
    return np.sin(np.pi / (count + 1) * turn) * (2.0 / (count + 1)) ** 0.5


def halves(table):
    table = np.asarray(table, np.float32)
    high = table.astype(BF16)
    return high, (table - high.astype(np.float32)).astype(BF16)


def wide(table):
    high, low = halves(table)
    return np.concatenate([high, low, high], axis=-1)


def split(values):
    high = values.astype(BF16)
    return high, (values - high.astype(F32)).astype(BF16)


def tall(values):
    high, low = split(values)
    return jnp.concatenate([high, high, low], axis=0)


def dot(a, b):
    return jnp.dot(a, b, preferred_element_type=F32)


def cost(flops, size):
    return pl.CostEstimate(flops=flops, bytes_accessed=size, transcendentals=0)


LIMIT = pltpu.CompilerParams(vmem_limit_bytes=24 * 1024 * 1024)


def vmem():
    return pl.BlockSpec(memory_space=pltpu.VMEM)


def x_kernel(even_ref, odd_ref, x_ref, a_ref, *refs):
    b_refs, (sums, diffs, held, sems) = refs[:DEEP], refs[DEEP:]
    half = x_ref.shape[0] // 2
    me = lax.axis_index("deep")
    step, steps = pl.program_id(0), held.shape[0]
    across = x_ref.shape[2] // 128

    def load(i):
        y, z = pl.multiple_of(i // across * 8, 8), pl.multiple_of(i % across * 128, 128)
        return pltpu.make_async_copy(x_ref.at[:, pl.ds(y, 8), pl.ds(z, 128)], held.at[i], sems.at[i])

    @pl.when(step == 0)
    def _():
        for i in range(steps):
            load(i).start()

    load(step).wait()

    def fold(t, carry):
        for j in range(32):
            i = t * 32 + j
            near, far = held[step, i], held[step, 2 * half - 1 - i]
            sums[pl.ds(pl.multiple_of(i * 8, 8), 8), :] = near + far
            diffs[pl.ds(pl.multiple_of(i * 8, 8), 8), :] = near - far
        return carry

    lax.fori_loop(0, half // 32, fold, 0)
    even = even_ref[...]
    odd = jnp.concatenate([odd_ref[me ^ k] for k in range(DEEP)], axis=0)
    a_rows = a_ref.reshape(half // 2 * 8, 128)
    b_rows = [b.reshape(NORTH * 8, 128) for b in b_refs]
    for y in range(0, 8, 2):
        s = jnp.concatenate([sums[pl.ds(y + j, half, stride=8), :] for j in range(2)], axis=1)
        e = dot(even, tall(s))
        t = jnp.concatenate([diffs[pl.ds(y + j, half, stride=8), :] for j in range(2)], axis=1)
        o = dot(odd, tall(t))
        for j in range(2):
            a_rows[pl.ds(y + j, half // 2, stride=8), :] = e[:, j * 128 : (j + 1) * 128]
            for k in range(DEEP):
                b_rows[k][pl.ds(y + j, NORTH, stride=8), :] = o[k * NORTH : (k + 1) * NORTH, j * 128 : (j + 1) * 128]


def x_stage(source):
    nx, ny, nz = source.shape
    modes = nx // 2
    block = modes // NORTH
    near = np.arange(nx // 2)
    even = wide(sines(near, np.arange(0, modes, 2), nx).T)
    odd_modes = (block * np.arange(NORTH)[None, :] + 2 * np.arange(DEEP)[:, None] + 1).reshape(-1)
    odd = wide(sines(near, odd_modes, nx).T).reshape(DEEP, NORTH, -1)
    across = nz // 128
    steps = ny // 8 * across
    b_shape = jax.ShapeDtypeStruct((NORTH, ny, nz), F32)
    b_spec = pl.BlockSpec((NORTH, 8, 128), lambda i: (0, i // across, i % across))
    return pl.pallas_call(
        x_kernel,
        grid=(steps,),
        in_specs=[vmem(), vmem(), pl.BlockSpec(memory_space=pl.ANY)],
        out_specs=[pl.BlockSpec((modes // 2, 8, 128), lambda i: (0, i // across, i % across))] + [b_spec] * DEEP,
        out_shape=[jax.ShapeDtypeStruct((modes // 2, ny, nz), F32)] + [b_shape] * DEEP,
        scratch_shapes=[pltpu.VMEM((nx // 2 * 8, 128), F32)] * 2
        + [pltpu.VMEM((steps, nx, 8, 128), F32), pltpu.SemaphoreType.DMA((steps,))],
        cost_estimate=cost(6 * nx * modes * ny * nz // 2, 6 * nx * ny * nz),
        name="x_stage",
    )(jnp.asarray(even), jnp.asarray(odd), source)


def y_table(ny):
    return jnp.asarray(wide(sines(np.arange(ny), np.arange(ny // 2), ny).T).reshape(DEEP, ny // 2 // DEEP, -1))


def ya_kernel(table_ref, v_ref, *outs):
    me = lax.axis_index("deep")
    table = jnp.concatenate([table_ref[me ^ k] for k in range(DEEP)], axis=0)
    v = v_ref[...]
    n, _, y, z = v.shape
    r = dot(table, tall(v.reshape(n * y, z)))
    m = r.shape[0] // DEEP
    for k in range(DEEP):
        outs[k][0] = r[k * m : (k + 1) * m]


def ya_stage(table, v):
    n, js, y, nz = v.shape
    m = table.shape[1]
    zb = 256
    return pl.pallas_call(
        ya_kernel,
        grid=(js, nz // zb),
        in_specs=[vmem(), pl.BlockSpec((n, 1, y, zb), lambda j, z: (0, j, 0, z))],
        out_specs=[pl.BlockSpec((1, m, zb), lambda j, z: (j, 0, z))] * DEEP,
        out_shape=[jax.ShapeDtypeStruct((js, m, nz), F32)] * DEEP,
        cost_estimate=cost(6 * n * y * m * DEEP * js * nz, 6 * n * js * y * nz),
        compiler_params=LIMIT,
        name="ya_stage",
    )(table, v)


def backwards(v):
    lanes = v.shape[-1] // 128
    at = 127 - lax.broadcasted_iota(jnp.int32, (v.shape[0], 128), 1)
    parts = [v[:, i * 128 : (i + 1) * 128] for i in range(lanes)]
    return jnp.concatenate([jnp.take_along_axis(p, at, axis=1) for p in parts[::-1]], axis=1)


def shuffled(even, odd):
    lane = lax.broadcasted_iota(jnp.int32, (even.shape[0], 128), 1)
    parts = []
    for i in range(even.shape[1] // 128):
        e, o = even[:, i * 128 : (i + 1) * 128], odd[:, i * 128 : (i + 1) * 128]
        for at in (lane // 2, lane // 2 + 64):
            e_at, o_at = jnp.take_along_axis(e, at, axis=1), jnp.take_along_axis(o, at, axis=1)
            parts.append(jnp.where(lane % 2 == 0, e_at, o_at))
    return jnp.concatenate(parts, axis=1)


def z_halves(near, far, table):
    far = backwards(far)
    count = near.shape[0]
    both = []
    for parity, v in enumerate((near + far, near - far)):
        high, low = split(v)
        r = dot(jnp.concatenate([high, low], axis=0), table[parity, 0])
        both.append(r[:count] + r[count:] + dot(high, table[parity, 1]))
    return both


def zb_kernel(table_ref, near_ref, far_ref, *rest):
    n, y, z = near_ref.shape
    even, odd = z_halves(near_ref[...].reshape(n * y, z), far_ref[...].reshape(n * y, z), table_ref)
    *before, o_ref = rest
    half = even.shape[1]
    even, odd = even.reshape(n, y, half), odd.reshape(n, y, half)
    if before:
        even, odd = even + before[0][:, :, :half], odd + before[0][:, :, half:]
    o_ref[:, :, :half] = even
    o_ref[:, :, half:] = odd


def zb_stage(table, near, far, *before):
    n, y, z = near.shape
    modes, rows = 2 * table.shape[3], 8
    spec = pl.BlockSpec((rows, y, z), lambda i: (i, 0, 0))
    wide_spec = pl.BlockSpec((rows, y, modes), lambda i: (i, 0, 0))
    return pl.pallas_call(
        zb_kernel,
        grid=(n // rows,),
        in_specs=[vmem(), spec, spec] + [wide_spec] * len(before),
        out_specs=wide_spec,
        out_shape=pltpu.HBM((n, y, modes), F32) if before else jax.ShapeDtypeStruct((n, y, modes), F32),
        cost_estimate=cost(6 * n * y * z * modes, 8 * n * y * (z + modes)),
        compiler_params=LIMIT,
        name="zb_stage",
    )(table, near, far, *before)


def za_kernel(sx_ref, t0_ref, t1_ref, sy_ref, sz_ref, p0, p1, p2, p3, o_ref):
    m, z = p0.shape[1], p0.shape[2]
    even0, odd0 = z_halves(p0[...].reshape(m, z), p3[...].reshape(m, z), t0_ref)
    even1, odd1 = z_halves(p1[...].reshape(m, z), p2[...].reshape(m, z), t1_ref)
    total = shuffled(even0 + even1, odd0 + odd1)
    yz = jnp.concatenate([sy_ref[lax.axis_index("deep")]] * (o_ref.shape[3] // 128), axis=1) + sz_ref[...]
    first = lax.axis_index("north") * 2 * pl.num_programs(0)
    o_ref[0, 0] = total * lax.rsqrt(sx_ref[first + 2 * pl.program_id(0)] + yz)


def za_stage(sx, tables, sy, sz, pieces):
    js, m, z = pieces[0].shape
    modes = 2 * tables[0].shape[3]
    spec = pl.BlockSpec((1, m, z), lambda j: (j, 0, 0))
    return pl.pallas_call(
        za_kernel,
        grid=(js,),
        in_specs=[pl.BlockSpec(memory_space=pltpu.SMEM)] + [vmem()] * 4 + [spec] * DEEP,
        out_specs=pl.BlockSpec((1, 1, m, modes), lambda j: (j, 0, 0, 0)),
        out_shape=jax.ShapeDtypeStruct((js, 2, m, modes), F32),
        cost_estimate=cost(6 * js * m * z * 2 * modes, 4 * js * m * z * DEEP + 8 * z * modes),
        compiler_params=LIMIT,
        name="za_stage",
    )(sx, *tables, sy, sz, *pieces)


def yb_kernel(sx_ref, table_ref, sy_ref, sz_ref, even_ref, odd_ref, *outs):
    me = lax.axis_index("deep")
    table = jnp.concatenate([table_ref[me ^ k] for k in range(DEEP)], axis=0)
    n, y, z = even_ref.shape
    e = dot(table, tall(even_ref[...].reshape(n * y, z)))
    o = dot(table, tall(odd_ref[...].reshape(n * y, z)))
    m = table.shape[0] // DEEP
    sx = sx_ref[lax.axis_index("north") * 2 * DEEP + 2 * me + 1]
    for k in range(DEEP):
        symbol = sx + jnp.concatenate([sy_ref[me ^ k]] * (2 * z // 128), axis=1) + sz_ref[...]
        outs[k][...] = shuffled(e[k * m : (k + 1) * m], o[k * m : (k + 1) * m]) * lax.rsqrt(symbol)


def yb_stage(sx, table, sy, sz, v):
    n, y, modes = v.shape
    m, block = table.shape[1], 512
    steps = modes // block
    return pl.pallas_call(
        yb_kernel,
        grid=(steps,),
        in_specs=[
            pl.BlockSpec(memory_space=pltpu.SMEM),
            vmem(),
            vmem(),
            pl.BlockSpec((1, block), lambda i: (0, i)),
            pl.BlockSpec((n, y, block // 2), lambda i: (0, 0, i)),
            pl.BlockSpec((n, y, block // 2), lambda i: (0, 0, i + 2)),
        ],
        out_specs=[pl.BlockSpec((m, block), lambda i: (0, i))] * DEEP,
        out_shape=[jax.ShapeDtypeStruct((m, modes), F32)] * DEEP,
        cost_estimate=cost(6 * n * y * m * DEEP * modes, 6 * n * y * modes),
        compiler_params=LIMIT,
        name="yb_stage",
    )(sx, table, sy, sz, v, v)


def join_kernel(whole_ref, p0, p1, p2, p3, o_ref, sems):
    me = lax.axis_index("deep")
    copies = [
        pltpu.make_async_copy(p, o_ref.at[me ^ k, 1], sems.at[k]) for k, p in enumerate((p0, p1, p2, p3))
    ]
    for copy in copies:
        copy.start()
    for copy in copies:
        copy.wait()


def join_stage(whole, pieces):
    return pl.pallas_call(
        join_kernel,
        in_specs=[pl.BlockSpec(memory_space=pl.ANY)] + [vmem()] * DEEP,
        out_specs=pl.BlockSpec(memory_space=pl.ANY),
        out_shape=jax.ShapeDtypeStruct(whole.shape, F32),
        scratch_shapes=[pltpu.SemaphoreType.DMA((DEEP,))],
        input_output_aliases={0: 0},
        cost_estimate=cost(1, 8 * pieces[0].size * DEEP),
        compiler_params=LIMIT,
        name="join_stage",
    )(whole, *pieces)


def z_table(count, pair):
    stretch = lax.axis_index("deep") ^ pair
    point = (stretch * (count // DEEP) + jnp.arange(count // DEEP))[None, :, None]
    mode = (2 * jnp.arange(count // 4) + jnp.arange(2)[:, None])[:, None, :]
    turn = (point + 1) * (mode + 1) % (2 * count + 2)
    table = jnp.sin(np.float32(np.pi / (count + 1)) * turn.astype(F32)) * np.float32((2.0 / (count + 1)) ** 0.5)
    high = lax.reduce_precision(table, 8, 7)
    return jnp.stack([high, table - high], axis=1).astype(BF16)


def deep_exchange(pieces):
    got = [pieces[0]] + [None] * (DEEP - 1)
    for k in (1, 3, 2):
        got[k] = lax.ppermute(pieces[k], "deep", [(s, s ^ k) for s in range(DEEP)])
    return got


def north_exchange(v):
    return lax.all_to_all(v, "north", split_axis=0, concat_axis=0, tiled=True)


def on_device(source, symbol_x, symbol_y, symbol_z):
    ny, nz = source.shape[1] * NORTH, source.shape[2] * DEEP
    a, *b = x_stage(source)
    b = deep_exchange(b)
    a = north_exchange(a.reshape(NORTH, -1, *a.shape[1:]))
    tz = [z_table(nz, q) for q in range(2)]
    ty = y_table(ny)
    sy = jnp.broadcast_to(symbol_y[: ny // 2, None], (ny // 2, 128)).reshape(DEEP, -1, 128)
    sz = symbol_z[None, : nz // 2]
    part = zb_stage(tz[0], b[0], b[3])
    part = zb_stage(tz[1], b[1], b[2], part)
    b = north_exchange(part)
    a = deep_exchange(ya_stage(ty, a))
    whole = za_stage(symbol_x, tz, sy, sz, a)
    b = deep_exchange(yb_stage(symbol_x, ty, sy, sz, b))
    whole = join_stage(whole, b)
    return whole.reshape(-1, *whole.shape[2:])


def solution(mesh):
    in_specs = (P(None, "north", "deep"), P(), P(), P())
    out_specs = P("north", "deep", None)
    return jax.shard_map(on_device, mesh=mesh, in_specs=in_specs, out_specs=out_specs, check_vma=False)
```

```python
import jax
import jax.numpy as jnp
import numpy as np
from jax import lax
from jax.experimental import pallas as pl
from jax.experimental.pallas import tpu as pltpu
from jax.sharding import PartitionSpec as P

F32, BF16 = jnp.float32, jnp.bfloat16
NORTH, DEEP = 32, 4


def sines(rows, modes, count):
    turn = np.outer(np.asarray(rows) + 1, np.asarray(modes) + 1) % (2 * count + 2)
    return np.sin(np.pi / (count + 1) * turn) * (2.0 / (count + 1)) ** 0.5


def halves(table):
    table = np.asarray(table, np.float32)
    high = table.astype(BF16)
    return high, (table - high.astype(np.float32)).astype(BF16)


def wide(table):
    high, low = halves(table)
    return np.concatenate([high, low, high], axis=-1)


def split(values):
    high = values.astype(BF16)
    return high, (values - high.astype(F32)).astype(BF16)


def tall(values):
    high, low = split(values)
    return jnp.concatenate([high, high, low], axis=0)


def dot(a, b):
    return jnp.dot(a, b, preferred_element_type=F32)


def product(table, values):
    count = table.shape[0] // 2
    high, low = split(values)
    r = dot(table, high)
    return r[:count] + r[count:] + dot(table[:count], low)


def cost(flops, size):
    return pl.CostEstimate(flops=flops, bytes_accessed=size, transcendentals=0)


LIMIT = pltpu.CompilerParams(vmem_limit_bytes=24 * 1024 * 1024)


def vmem():
    return pl.BlockSpec(memory_space=pltpu.VMEM)


def upside_down(v):
    at = 7 - lax.broadcasted_iota(jnp.int32, (8, v.shape[1]), 0)
    parts = [jnp.take_along_axis(v[i : i + 8], at, axis=0) for i in range(0, v.shape[0], 8)]
    return jnp.concatenate(parts[::-1], axis=0)


def x_kernel(even_ref, odd_ref, x_ref, a_ref, *refs):
    b_refs, (held, sems) = refs[:DEEP], refs[DEEP:]
    half = x_ref.shape[0] // 2
    me = lax.axis_index("deep")
    step, steps, slots = pl.program_id(0), pl.num_programs(0), held.shape[0]
    across = x_ref.shape[2] // 128

    def load(i):
        y, z = pl.multiple_of(i // across * 8, 8), pl.multiple_of(i % across * 128, 128)
        slot = lax.rem(i, slots)
        return pltpu.make_async_copy(x_ref.at[:, pl.ds(y, 8), pl.ds(z, 128)], held.at[slot], sems.at[slot])

    @pl.when(step == 0)
    def _():
        for i in range(slots):
            load(i).start()

    load(step).wait()
    even = even_ref[...].reshape(half, half)
    odd = jnp.concatenate([odd_ref[h, me ^ k] for h in range(2) for k in range(DEEP)], axis=0)
    a_rows = a_ref.reshape(half // 2 * 8, 128)
    b_rows = [b.reshape(NORTH * 8, 128) for b in b_refs]
    rows = held.reshape(slots * half * 2 * 8, 128)
    base = lax.rem(step, slots) * half * 2 * 8

    for y in range(0, 8, 2):
        near, far = (
            jnp.concatenate(
                [rows[pl.ds(base + first * half * 8 + y + j, half, stride=8), :] for j in range(2)], axis=1
            )
            for first in range(2)
        )
        far = upside_down(far)
        e = product(even, near + far)
        o = product(odd, near - far)
        for j in range(2):
            lanes = slice(j * 128, j * 128 + 128)
            a_rows[pl.ds(y + j, half // 2, stride=8), :] = e[:, lanes]
            for k in range(DEEP):
                b_rows[k][pl.ds(y + j, NORTH, stride=8), :] = o[k * NORTH : (k + 1) * NORTH, lanes]

    @pl.when(step + slots < steps)
    def _():
        load(step + slots).start()


def x_stage(source):
    nx, ny, nz = source.shape
    modes = nx // 2
    block = modes // NORTH
    near = np.arange(nx // 2)
    even = np.stack(halves(sines(near, np.arange(0, modes, 2), nx).T))
    odd_modes = (block * np.arange(NORTH)[None, :] + 2 * np.arange(DEEP)[:, None] + 1).reshape(-1)
    odd = np.stack(halves(sines(near, odd_modes, nx).T)).reshape(2, DEEP, NORTH, -1)
    across = nz // 128
    steps = ny // 8 * across
    b_shape = jax.ShapeDtypeStruct((NORTH, ny, nz), F32)
    b_spec = pl.BlockSpec((NORTH, 8, 128), lambda i: (0, i // across, i % across))
    return pl.pallas_call(
        x_kernel,
        grid=(steps,),
        in_specs=[vmem(), vmem(), pl.BlockSpec(memory_space=pl.ANY)],
        out_specs=[pl.BlockSpec((modes // 2, 8, 128), lambda i: (0, i // across, i % across))] + [b_spec] * DEEP,
        out_shape=[jax.ShapeDtypeStruct((modes // 2, ny, nz), F32)] + [b_shape] * DEEP,
        scratch_shapes=[pltpu.VMEM((4, nx, 8, 128), F32), pltpu.SemaphoreType.DMA((4,))],
        cost_estimate=cost(6 * nx * modes * ny * nz // 2, 6 * nx * ny * nz),
        name="x_stage",
    )(jnp.asarray(even), jnp.asarray(odd), source)


def y_table(ny):
    return jnp.asarray(wide(sines(np.arange(ny), np.arange(ny // 2), ny).T).reshape(DEEP, ny // 2 // DEEP, -1))


def ya_kernel(table_ref, v_ref, *refs):
    outs, (held, sems) = refs[:DEEP], refs[DEEP:]
    me, j = lax.axis_index("deep"), pl.program_id(0)

    def load(i):
        return pltpu.make_async_copy(v_ref.at[:, i], held.at[i], sems.at[i])

    @pl.when(j == 0)
    def _():
        for i in range(held.shape[0]):
            load(i).start()

    load(j).wait()
    table = jnp.concatenate([table_ref[me ^ k] for k in range(DEEP)], axis=0)
    n, y, z = held.shape[1:]
    m, block = table.shape[0] // DEEP, 256
    for i in range(z // block):
        at = slice(i * block, (i + 1) * block)
        r = dot(table, tall(held[j, :, :, at].reshape(n * y, block)))
        for k in range(DEEP):
            outs[k][0, :, at] = r[k * m : (k + 1) * m]


def ya_stage(table, v):
    n, js, y, nz = v.shape
    m = table.shape[1]
    return pl.pallas_call(
        ya_kernel,
        grid=(js,),
        in_specs=[vmem(), pl.BlockSpec(memory_space=pltpu.HBM)],
        out_specs=[pl.BlockSpec((1, m, nz), lambda j: (j, 0, 0))] * DEEP,
        out_shape=[jax.ShapeDtypeStruct((js, m, nz), F32)] * DEEP,
        scratch_shapes=[pltpu.VMEM((js, n, y, nz), F32), pltpu.SemaphoreType.DMA((js,))],
        cost_estimate=cost(6 * n * y * m * DEEP * js * nz, 6 * n * js * y * nz),
        compiler_params=LIMIT,
        name="ya_stage",
    )(table, v)


def backwards(v):
    lanes = v.shape[-1] // 128
    at = 127 - lax.broadcasted_iota(jnp.int32, (v.shape[0], 128), 1)
    parts = [v[:, i * 128 : (i + 1) * 128] for i in range(lanes)]
    return jnp.concatenate([jnp.take_along_axis(p, at, axis=1) for p in parts[::-1]], axis=1)


def shuffled(even, odd):
    lane = lax.broadcasted_iota(jnp.int32, (even.shape[0], 128), 1)
    parts = []
    for i in range(even.shape[1] // 128):
        e, o = even[:, i * 128 : (i + 1) * 128], odd[:, i * 128 : (i + 1) * 128]
        for at in (lane // 2, lane // 2 + 64):
            e_at, o_at = jnp.take_along_axis(e, at, axis=1), jnp.take_along_axis(o, at, axis=1)
            parts.append(jnp.where(lane % 2 == 0, e_at, o_at))
    return jnp.concatenate(parts, axis=1)


def z_halves(near, far, table):
    far = backwards(far)
    count = near.shape[0]
    both = []
    for parity, v in enumerate((near + far, near - far)):
        high, low = split(v)
        r = dot(jnp.concatenate([high, low], axis=0), table[parity, 0])
        both.append(r[:count] + r[count:] + dot(high, table[parity, 1]))
    return both


def zb_rows(table_ref, near, far, before, o_ref):
    n, y, z = near.shape
    both = z_halves(near.reshape(n * y, z), far.reshape(n * y, z), table_ref)
    for i in range(o_ref.shape[1]):
        for p in range(2):
            r = both[p][:, i * 128 : (i + 1) * 128].reshape(n, y, 128)
            lanes = slice(p * 128, p * 128 + 128)
            o_ref[:, i, :, lanes] = r if before is None else r + before[:, i, :, lanes]


def zb1_kernel(table_ref, near_ref, far_ref, o_ref):
    zb_rows(table_ref, near_ref[...], far_ref[...], None, o_ref)


def zb2_kernel(table_ref, before_ref, near_ref, far_ref, o_ref, near, far, sems):
    step = pl.program_id(0)
    rows = o_ref.shape[0]

    def loads(i):
        return [
            pltpu.make_async_copy(ref.at[pl.ds(i * rows, rows)], held.at[pl.ds(i * rows, rows)], sems.at[i, k])
            for k, (ref, held) in enumerate(((near_ref, near), (far_ref, far)))
        ]

    @pl.when(step == 0)
    def _():
        for i in range(near.shape[0] // rows):
            for copy in loads(i):
                copy.start()

    for copy in loads(step):
        copy.wait()
    at = pl.ds(step * rows, rows)
    zb_rows(table_ref, near[at], far[at], before_ref, o_ref)


def zb_stage(table, near, far, before=None):
    n, y, z = near.shape
    modes, rows = 2 * table.shape[3], 8
    spec = pl.BlockSpec((rows, y, z), lambda i: (i, 0, 0))
    wide_spec = pl.BlockSpec((rows, modes // 256, y, 256), lambda i: (i, 0, 0, 0))
    hbm = pl.BlockSpec(memory_space=pltpu.HBM)
    first = before is None
    shape = (n, modes // 256, y, 256)
    return pl.pallas_call(
        zb1_kernel if first else zb2_kernel,
        grid=(n // rows,),
        in_specs=[vmem(), spec, spec] if first else [vmem(), wide_spec, hbm, hbm],
        out_specs=wide_spec,
        out_shape=jax.ShapeDtypeStruct(shape, F32) if first else pltpu.HBM(shape, F32),
        scratch_shapes=[]
        if first
        else [pltpu.VMEM((n, y, z), F32)] * 2 + [pltpu.SemaphoreType.DMA((n // rows, 2))],
        cost_estimate=cost(6 * n * y * z * modes, 8 * n * y * (z + modes)),
        compiler_params=LIMIT,
        name="zb_stage",
    )(*((table, near, far) if first else (table, before, near, far)))


def za_kernel(sx_ref, t0_ref, t1_ref, sy_ref, sz_ref, p0, p1, p2, p3, o_ref):
    m, z = p0.shape[1], p0.shape[2]
    even0, odd0 = z_halves(p0[...].reshape(m, z), p3[...].reshape(m, z), t0_ref)
    even1, odd1 = z_halves(p1[...].reshape(m, z), p2[...].reshape(m, z), t1_ref)
    total = shuffled(even0 + even1, odd0 + odd1)
    yz = jnp.concatenate([sy_ref[lax.axis_index("deep")]] * (o_ref.shape[3] // 128), axis=1) + sz_ref[...]
    first = lax.axis_index("north") * 2 * pl.num_programs(0)
    o_ref[0, 0] = total * lax.rsqrt(sx_ref[first + 2 * pl.program_id(0)] + yz)


def za_stage(sx, tables, sy, sz, pieces):
    js, m, z = pieces[0].shape
    modes = 2 * tables[0].shape[3]
    spec = pl.BlockSpec((1, m, z), lambda j: (j, 0, 0))
    return pl.pallas_call(
        za_kernel,
        grid=(js,),
        in_specs=[pl.BlockSpec(memory_space=pltpu.SMEM)] + [vmem()] * 4 + [spec] * DEEP,
        out_specs=pl.BlockSpec((1, 1, m, modes), lambda j: (j, 0, 0, 0)),
        out_shape=jax.ShapeDtypeStruct((js, 2, m, modes), F32),
        cost_estimate=cost(6 * js * m * z * 2 * modes, 4 * js * m * z * DEEP + 8 * z * modes),
        compiler_params=LIMIT,
        name="za_stage",
    )(sx, *tables, sy, sz, *pieces)


def yb_kernel(sx_ref, table_ref, sy_ref, sz_ref, v_ref, *outs):
    me = lax.axis_index("deep")
    n, _, y, block = v_ref.shape
    table = jnp.concatenate([table_ref[me ^ k] for k in range(DEEP)], axis=0)
    r = dot(table, tall(v_ref[...].reshape(n * y, block)))
    m = table.shape[0] // DEEP
    sx = sx_ref[lax.axis_index("north") * 2 * DEEP + 2 * me + 1]
    for k in range(DEEP):
        symbol = sx + jnp.concatenate([sy_ref[me ^ k]] * (block // 128), axis=1) + sz_ref[...]
        rows = slice(k * m, (k + 1) * m)
        outs[k][...] = shuffled(r[rows, : block // 2], r[rows, block // 2 :]) * lax.rsqrt(symbol)


def yb_stage(sx, table, sy, sz, v):
    n, steps, y, block = v.shape
    m = table.shape[1]
    modes = steps * block
    return pl.pallas_call(
        yb_kernel,
        grid=(steps,),
        in_specs=[
            pl.BlockSpec(memory_space=pltpu.SMEM),
            vmem(),
            vmem(),
            pl.BlockSpec((1, block), lambda i: (0, i)),
            pl.BlockSpec((n, 1, y, block), lambda i: (0, i, 0, 0)),
        ],
        out_specs=[pl.BlockSpec((m, block), lambda i: (0, i))] * DEEP,
        out_shape=[jax.ShapeDtypeStruct((m, modes), F32)] * DEEP,
        cost_estimate=cost(6 * n * y * m * DEEP * modes, 6 * n * y * modes),
        compiler_params=LIMIT,
        name="yb_stage",
    )(sx, table, sy, sz, v)


def join_kernel(whole_ref, p0, p1, p2, p3, o_ref, sems):
    me = lax.axis_index("deep")
    copies = [
        pltpu.make_async_copy(p, o_ref.at[me ^ k, 1], sems.at[k]) for k, p in enumerate((p0, p1, p2, p3))
    ]
    for copy in copies:
        copy.start()
    for copy in copies:
        copy.wait()


def join_stage(whole, pieces):
    return pl.pallas_call(
        join_kernel,
        in_specs=[pl.BlockSpec(memory_space=pl.ANY)] + [vmem()] * DEEP,
        out_specs=pl.BlockSpec(memory_space=pl.ANY),
        out_shape=jax.ShapeDtypeStruct(whole.shape, F32),
        scratch_shapes=[pltpu.SemaphoreType.DMA((DEEP,))],
        input_output_aliases={0: 0},
        cost_estimate=cost(1, 8 * pieces[0].size * DEEP),
        compiler_params=LIMIT,
        name="join_stage",
    )(whole, *pieces)


def z_table(count, pair):
    stretch = lax.axis_index("deep") ^ pair
    point = (stretch * (count // DEEP) + jnp.arange(count // DEEP))[None, :, None]
    mode = (2 * jnp.arange(count // 4) + jnp.arange(2)[:, None])[:, None, :]
    turn = (point + 1) * (mode + 1) % (2 * count + 2)
    table = jnp.sin(np.float32(np.pi / (count + 1)) * turn.astype(F32)) * np.float32((2.0 / (count + 1)) ** 0.5)
    high = lax.reduce_precision(table, 8, 7)
    return jnp.stack([high, table - high], axis=1).astype(BF16)


def deep_exchange(pieces):
    got = [pieces[0]] + [None] * (DEEP - 1)
    for k in (1, 3, 2):
        got[k] = lax.ppermute(pieces[k], "deep", [(s, s ^ k) for s in range(DEEP)])
    return got


def north_exchange(v):
    return lax.all_to_all(v, "north", split_axis=0, concat_axis=0, tiled=True)


def on_device(source, symbol_x, symbol_y, symbol_z):
    ny, nz = source.shape[1] * NORTH, source.shape[2] * DEEP
    a, *b = x_stage(source)
    b = deep_exchange(b)
    a = north_exchange(a.reshape(NORTH, -1, *a.shape[1:]))
    tz = [z_table(nz, q) for q in range(2)]
    ty = y_table(ny)
    sy = jnp.broadcast_to(symbol_y[: ny // 2, None], (ny // 2, 128)).reshape(DEEP, -1, 128)
    sz = symbol_z[None, : nz // 2]
    part = zb_stage(tz[0], b[0], b[3])
    part = zb_stage(tz[1], b[1], b[2], part)
    b = north_exchange(part)
    a = deep_exchange(ya_stage(ty, a))
    whole = za_stage(symbol_x, tz, sy, sz, a)
    b = deep_exchange(yb_stage(symbol_x, ty, sy, sz, b))
    whole = join_stage(whole, b)
    return whole.reshape(-1, *whole.shape[2:])


def solution(mesh):
    in_specs = (P(None, "north", "deep"), P(), P(), P())
    out_specs = P("north", "deep", None)
    return jax.shard_map(on_device, mesh=mesh, in_specs=in_specs, out_specs=out_specs, check_vma=False)
```

```python
import jax
import jax.numpy as jnp
import numpy as np
from jax import lax
from jax.experimental import pallas as pl
from jax.experimental.pallas import tpu as pltpu
from jax.sharding import PartitionSpec as P

F32, BF16 = jnp.float32, jnp.bfloat16
NORTH, DEEP = 32, 4


def sines(rows, modes, count):
    turn = np.outer(np.asarray(rows) + 1, np.asarray(modes) + 1) % (2 * count + 2)
    return np.sin(np.pi / (count + 1) * turn) * (2.0 / (count + 1)) ** 0.5


def halves(table):
    table = np.asarray(table, np.float32)
    high = table.astype(BF16)
    return high, (table - high.astype(np.float32)).astype(BF16)


def wide(table):
    high, low = halves(table)
    return np.concatenate([high, low, high], axis=-1)


def split(values):
    high = values.astype(BF16)
    return high, (values - high.astype(F32)).astype(BF16)


def tall(values):
    high, low = split(values)
    return jnp.concatenate([high, high, low], axis=0)


def dot(a, b):
    return jnp.dot(a, b, preferred_element_type=F32)


def product(table, values):
    count = table.shape[0] // 2
    high, low = split(values)
    r = dot(table, high)
    return r[:count] + r[count:] + dot(table[:count], low)


def cost(flops, size):
    return pl.CostEstimate(flops=flops, bytes_accessed=size, transcendentals=0)


LIMIT = pltpu.CompilerParams(vmem_limit_bytes=24 * 1024 * 1024)


def vmem():
    return pl.BlockSpec(memory_space=pltpu.VMEM)


def upside_down(v):
    at = 7 - lax.broadcasted_iota(jnp.int32, (8, v.shape[1]), 0)
    parts = [jnp.take_along_axis(v[i : i + 8], at, axis=0) for i in range(0, v.shape[0], 8)]
    return jnp.concatenate(parts[::-1], axis=0)


def x_kernel(even_ref, odd_ref, x_ref, a_ref, *refs):
    b_refs, (held, sems) = refs[:DEEP], refs[DEEP:]
    half = x_ref.shape[0] // 2
    me = lax.axis_index("deep")
    step, steps, slots = pl.program_id(0), pl.num_programs(0), held.shape[0]
    across = x_ref.shape[2] // 128

    def load(i):
        y, z = pl.multiple_of(i // across * 8, 8), pl.multiple_of(i % across * 128, 128)
        slot = lax.rem(i, slots)
        return pltpu.make_async_copy(x_ref.at[:, pl.ds(y, 8), pl.ds(z, 128)], held.at[slot], sems.at[slot])

    @pl.when(step == 0)
    def _():
        for i in range(slots):
            load(i).start()

    load(step).wait()
    even = even_ref[...].reshape(half, half)
    odd = jnp.concatenate([odd_ref[h, me ^ k] for h in range(2) for k in range(DEEP)], axis=0)
    a_rows = a_ref.reshape(half // 2 * 8, 128)
    b_rows = [b.reshape(NORTH * 8, 128) for b in b_refs]
    rows = held.reshape(slots * half * 2 * 8, 128)
    base = lax.rem(step, slots) * half * 2 * 8

    for y in range(0, 8, 2):
        near, far = (
            jnp.concatenate(
                [rows[pl.ds(base + first * half * 8 + y + j, half, stride=8), :] for j in range(2)], axis=1
            )
            for first in range(2)
        )
        far = upside_down(far)
        e = product(even, near + far)
        o = product(odd, near - far)
        for j in range(2):
            lanes = slice(j * 128, j * 128 + 128)
            a_rows[pl.ds(y + j, half // 2, stride=8), :] = e[:, lanes]
            for k in range(DEEP):
                b_rows[k][pl.ds(y + j, NORTH, stride=8), :] = o[k * NORTH : (k + 1) * NORTH, lanes]

    @pl.when(step + slots < steps)
    def _():
        load(step + slots).start()


def x_stage(source):
    nx, ny, nz = source.shape
    modes = nx // 2
    block = modes // NORTH
    near = np.arange(nx // 2)
    even = np.stack(halves(sines(near, np.arange(0, modes, 2), nx).T))
    odd_modes = (block * np.arange(NORTH)[None, :] + 2 * np.arange(DEEP)[:, None] + 1).reshape(-1)
    odd = np.stack(halves(sines(near, odd_modes, nx).T)).reshape(2, DEEP, NORTH, -1)
    across = nz // 128
    steps = ny // 8 * across
    b_shape = jax.ShapeDtypeStruct((NORTH, ny, nz), F32)
    b_spec = pl.BlockSpec((NORTH, 8, 128), lambda i: (0, i // across, i % across))
    return pl.pallas_call(
        x_kernel,
        grid=(steps,),
        in_specs=[vmem(), vmem(), pl.BlockSpec(memory_space=pl.ANY)],
        out_specs=[pl.BlockSpec((modes // 2, 8, 128), lambda i: (0, i // across, i % across))] + [b_spec] * DEEP,
        out_shape=[jax.ShapeDtypeStruct((modes // 2, ny, nz), F32)] + [b_shape] * DEEP,
        scratch_shapes=[pltpu.VMEM((4, nx, 8, 128), F32), pltpu.SemaphoreType.DMA((4,))],
        cost_estimate=cost(6 * nx * modes * ny * nz // 2, 6 * nx * ny * nz),
        name="x_stage",
    )(jnp.asarray(even), jnp.asarray(odd), source)


def y_table(ny):
    return jnp.asarray(wide(sines(np.arange(ny), np.arange(ny // 2), ny).T).reshape(DEEP, ny // 2 // DEEP, -1))


def ya_kernel(table_ref, v_ref, *refs):
    outs, (held, sems) = refs[:DEEP], refs[DEEP:]
    me, j = lax.axis_index("deep"), pl.program_id(0)

    def load(i):
        return pltpu.make_async_copy(v_ref.at[:, i], held.at[i], sems.at[i])

    @pl.when(j == 0)
    def _():
        for i in range(held.shape[0]):
            load(i).start()

    load(j).wait()
    table = jnp.concatenate([table_ref[me ^ k] for k in range(DEEP)], axis=0)
    n, y, z = held.shape[1:]
    m, block = table.shape[0] // DEEP, 256
    for i in range(z // block):
        at = slice(i * block, (i + 1) * block)
        r = dot(table, tall(held[j, :, :, at].reshape(n * y, block)))
        for k in range(DEEP):
            outs[k][0, :, at] = r[k * m : (k + 1) * m]


def ya_stage(table, v):
    n, js, y, nz = v.shape
    m = table.shape[1]
    return pl.pallas_call(
        ya_kernel,
        grid=(js,),
        in_specs=[vmem(), pl.BlockSpec(memory_space=pltpu.HBM)],
        out_specs=[pl.BlockSpec((1, m, nz), lambda j: (j, 0, 0))] * DEEP,
        out_shape=[jax.ShapeDtypeStruct((js, m, nz), F32)] * DEEP,
        scratch_shapes=[pltpu.VMEM((js, n, y, nz), F32), pltpu.SemaphoreType.DMA((js,))],
        cost_estimate=cost(6 * n * y * m * DEEP * js * nz, 6 * n * js * y * nz),
        compiler_params=LIMIT,
        name="ya_stage",
    )(table, v)


def backwards(v):
    lanes = v.shape[-1] // 128
    at = 127 - lax.broadcasted_iota(jnp.int32, (v.shape[0], 128), 1)
    parts = [v[:, i * 128 : (i + 1) * 128] for i in range(lanes)]
    return jnp.concatenate([jnp.take_along_axis(p, at, axis=1) for p in parts[::-1]], axis=1)


def shuffled(even, odd):
    lane = lax.broadcasted_iota(jnp.int32, (even.shape[0], 128), 1)
    parts = []
    for i in range(even.shape[1] // 128):
        e, o = even[:, i * 128 : (i + 1) * 128], odd[:, i * 128 : (i + 1) * 128]
        for at in (lane // 2, lane // 2 + 64):
            e_at, o_at = jnp.take_along_axis(e, at, axis=1), jnp.take_along_axis(o, at, axis=1)
            parts.append(jnp.where(lane % 2 == 0, e_at, o_at))
    return jnp.concatenate(parts, axis=1)


def z_halves(near, far, table):
    far = backwards(far)
    count = near.shape[0]
    both = []
    for parity, v in enumerate((near + far, near - far)):
        high, low = split(v)
        r = dot(jnp.concatenate([high, low], axis=0), table[parity, 0])
        both.append(r[:count] + r[count:] + dot(high, table[parity, 1]))
    return both


def zb_rows(table_ref, near, far, before, o_ref):
    n, y, z = near.shape
    both = z_halves(near.reshape(n * y, z), far.reshape(n * y, z), table_ref)
    for i in range(o_ref.shape[1]):
        for p in range(2):
            r = both[p][:, i * 128 : (i + 1) * 128].reshape(n, y, 128)
            lanes = slice(p * 128, p * 128 + 128)
            o_ref[:, i, :, lanes] = r if before is None else r + before[:, i, :, lanes]


def zb1_kernel(table_ref, near_ref, far_ref, o_ref):
    zb_rows(table_ref, near_ref[...], far_ref[...], None, o_ref)


def zb2_kernel(table_ref, before_ref, near_ref, far_ref, o_ref, near, far, sems):
    step = pl.program_id(0)
    rows = o_ref.shape[0]

    def loads(i):
        return [
            pltpu.make_async_copy(ref.at[pl.ds(i * rows, rows)], held.at[pl.ds(i * rows, rows)], sems.at[i, k])
            for k, (ref, held) in enumerate(((near_ref, near), (far_ref, far)))
        ]

    @pl.when(step == 0)
    def _():
        for i in range(near.shape[0] // rows):
            for copy in loads(i):
                copy.start()

    for copy in loads(step):
        copy.wait()
    at = pl.ds(step * rows, rows)
    zb_rows(table_ref, near[at], far[at], before_ref, o_ref)


def zb_stage(table, near, far, before=None):
    n, y, z = near.shape
    modes, rows = 2 * table.shape[3], 8
    spec = pl.BlockSpec((rows, y, z), lambda i: (i, 0, 0))
    wide_spec = pl.BlockSpec((rows, modes // 256, y, 256), lambda i: (i, 0, 0, 0))
    hbm = pl.BlockSpec(memory_space=pltpu.HBM)
    first = before is None
    shape = (n, modes // 256, y, 256)
    return pl.pallas_call(
        zb1_kernel if first else zb2_kernel,
        grid=(n // rows,),
        in_specs=[vmem(), spec, spec] if first else [vmem(), wide_spec, hbm, hbm],
        out_specs=wide_spec,
        out_shape=jax.ShapeDtypeStruct(shape, F32) if first else pltpu.HBM(shape, F32),
        scratch_shapes=[]
        if first
        else [pltpu.VMEM((n, y, z), F32)] * 2 + [pltpu.SemaphoreType.DMA((n // rows, 2))],
        cost_estimate=cost(6 * n * y * z * modes, 8 * n * y * (z + modes)),
        compiler_params=LIMIT,
        name="zb_stage",
    )(*((table, near, far) if first else (table, before, near, far)))


def za_kernel(sx_ref, t0_ref, t1_ref, sy_ref, sz_ref, p0, p1, p2, p3, o_ref):
    m, z = p0.shape[1], p0.shape[2]
    even0, odd0 = z_halves(p0[...].reshape(m, z), p3[...].reshape(m, z), t0_ref)
    even1, odd1 = z_halves(p1[...].reshape(m, z), p2[...].reshape(m, z), t1_ref)
    total = shuffled(even0 + even1, odd0 + odd1)
    yz = jnp.concatenate([sy_ref[lax.axis_index("deep")]] * (o_ref.shape[3] // 128), axis=1) + sz_ref[...]
    first = lax.axis_index("north") * 2 * pl.num_programs(0)
    o_ref[0, 0] = total * lax.rsqrt(sx_ref[first + 2 * pl.program_id(0)] + yz)


def za_stage(sx, tables, sy, sz, pieces):
    js, m, z = pieces[0].shape
    modes = 2 * tables[0].shape[3]
    spec = pl.BlockSpec((1, m, z), lambda j: (j, 0, 0))
    return pl.pallas_call(
        za_kernel,
        grid=(js,),
        in_specs=[pl.BlockSpec(memory_space=pltpu.SMEM)] + [vmem()] * 4 + [spec] * DEEP,
        out_specs=pl.BlockSpec((1, 1, m, modes), lambda j: (j, 0, 0, 0)),
        out_shape=jax.ShapeDtypeStruct((js, 2, m, modes), F32),
        cost_estimate=cost(6 * js * m * z * 2 * modes, 4 * js * m * z * DEEP + 8 * z * modes),
        compiler_params=LIMIT,
        name="za_stage",
    )(sx, *tables, sy, sz, *pieces)


def yb_kernel(sx_ref, table_ref, sy_ref, sz_ref, v_ref, *outs):
    me = lax.axis_index("deep")
    n, blocks, y, block = v_ref.shape
    table = jnp.concatenate([table_ref[me ^ k] for k in range(DEEP)], axis=0)
    m = table.shape[0] // DEEP
    sx = sx_ref[lax.axis_index("north") * 2 * DEEP + 2 * me + 1]
    for b in range(blocks):
        r = dot(table, tall(v_ref[:, b].reshape(n * y, block)))
        lanes = slice(b * block, (b + 1) * block)
        for k in range(DEEP):
            symbol = sx + jnp.concatenate([sy_ref[me ^ k]] * (block // 128), axis=1) + sz_ref[:, lanes]
            rows = slice(k * m, (k + 1) * m)
            outs[k][:, lanes] = shuffled(r[rows, : block // 2], r[rows, block // 2 :]) * lax.rsqrt(symbol)


def yb_stage(sx, table, sy, sz, v):
    n, blocks, y, block = v.shape
    m = table.shape[1]
    modes, steps = blocks * block, 2
    return pl.pallas_call(
        yb_kernel,
        grid=(steps,),
        in_specs=[
            pl.BlockSpec(memory_space=pltpu.SMEM),
            vmem(),
            vmem(),
            pl.BlockSpec((1, modes // steps), lambda i: (0, i)),
            pl.BlockSpec((n, blocks // steps, y, block), lambda i: (0, i, 0, 0)),
        ],
        out_specs=[pl.BlockSpec((m, modes // steps), lambda i: (0, i))] * DEEP,
        out_shape=[jax.ShapeDtypeStruct((m, modes), F32)] * DEEP,
        cost_estimate=cost(6 * n * y * m * DEEP * modes, 6 * n * y * modes),
        compiler_params=LIMIT,
        name="yb_stage",
    )(sx, table, sy, sz, v)


def join_kernel(whole_ref, p0, p1, p2, p3, o_ref, sems):
    me = lax.axis_index("deep")
    copies = [
        pltpu.make_async_copy(p, o_ref.at[me ^ k, 1], sems.at[k]) for k, p in enumerate((p0, p1, p2, p3))
    ]
    for copy in copies:
        copy.start()
    for copy in copies:
        copy.wait()


def join_stage(whole, pieces):
    return pl.pallas_call(
        join_kernel,
        in_specs=[pl.BlockSpec(memory_space=pl.ANY)] + [vmem()] * DEEP,
        out_specs=pl.BlockSpec(memory_space=pl.ANY),
        out_shape=jax.ShapeDtypeStruct(whole.shape, F32),
        scratch_shapes=[pltpu.SemaphoreType.DMA((DEEP,))],
        input_output_aliases={0: 0},
        cost_estimate=cost(1, 8 * pieces[0].size * DEEP),
        compiler_params=LIMIT,
        name="join_stage",
    )(whole, *pieces)


def z_table(count, pair):
    stretch = lax.axis_index("deep") ^ pair
    point = (stretch * (count // DEEP) + jnp.arange(count // DEEP))[None, :, None]
    mode = (2 * jnp.arange(count // 4) + jnp.arange(2)[:, None])[:, None, :]
    turn = (point + 1) * (mode + 1) % (2 * count + 2)
    table = jnp.sin(np.float32(np.pi / (count + 1)) * turn.astype(F32)) * np.float32((2.0 / (count + 1)) ** 0.5)
    high = lax.reduce_precision(table, 8, 7)
    return jnp.stack([high, table - high], axis=1).astype(BF16)


def deep_exchange(pieces):
    got = [pieces[0]] + [None] * (DEEP - 1)
    for k in (1, 3, 2):
        got[k] = lax.ppermute(pieces[k], "deep", [(s, s ^ k) for s in range(DEEP)])
    return got


def north_exchange(v):
    return lax.all_to_all(v, "north", split_axis=0, concat_axis=0, tiled=True)


def on_device(source, symbol_x, symbol_y, symbol_z):
    ny, nz = source.shape[1] * NORTH, source.shape[2] * DEEP
    a, *b = x_stage(source)
    b = deep_exchange(b)
    a = north_exchange(a.reshape(NORTH, -1, *a.shape[1:]))
    tz = [z_table(nz, q) for q in range(2)]
    ty = y_table(ny)
    sy = jnp.broadcast_to(symbol_y[: ny // 2, None], (ny // 2, 128)).reshape(DEEP, -1, 128)
    sz = symbol_z[None, : nz // 2]
    part = zb_stage(tz[0], b[0], b[3])
    part = zb_stage(tz[1], b[1], b[2], part)
    b = north_exchange(part)
    a = deep_exchange(ya_stage(ty, a))
    whole = za_stage(symbol_x, tz, sy, sz, a)
    b = deep_exchange(yb_stage(symbol_x, ty, sy, sz, b))
    whole = join_stage(whole, b)
    return whole.reshape(-1, *whole.shape[2:])


def solution(mesh):
    in_specs = (P(None, "north", "deep"), P(), P(), P())
    out_specs = P("north", "deep", None)
    return jax.shard_map(on_device, mesh=mesh, in_specs=in_specs, out_specs=out_specs, check_vma=False)
```

```python
import functools

import jax
import jax.numpy as jnp
import numpy as np
from jax import lax
from jax.experimental import pallas as pl
from jax.experimental.pallas import tpu as pltpu
from jax.sharding import PartitionSpec as P

F32, BF16 = jnp.float32, jnp.bfloat16
NORTH, DEEP = 32, 4


def sines(rows, modes, count):
    turn = np.outer(np.asarray(rows) + 1, np.asarray(modes) + 1) % (2 * count + 2)
    return np.sin(np.pi / (count + 1) * turn) * (2.0 / (count + 1)) ** 0.5


def halves(table):
    table = np.asarray(table, np.float32)
    high = table.astype(BF16)
    return high, (table - high.astype(np.float32)).astype(BF16)


def wide(table):
    high, low = halves(table)
    return np.concatenate([high, low, high], axis=-1)


def split(values):
    high = values.astype(BF16)
    return high, (values - high.astype(F32)).astype(BF16)


def tall(values):
    high, low = split(values)
    return jnp.concatenate([high, high, low], axis=0)


def dot(a, b):
    return jnp.dot(a, b, preferred_element_type=F32)


def product(table, values):
    count = table.shape[0] // 2
    high, low = split(values)
    r = dot(table, high)
    return r[:count] + r[count:] + dot(table[:count], low)


def cost(flops, size):
    return pl.CostEstimate(flops=flops, bytes_accessed=size, transcendentals=0)


LIMIT = pltpu.CompilerParams(vmem_limit_bytes=24 * 1024 * 1024)


def vmem():
    return pl.BlockSpec(memory_space=pltpu.VMEM)


def upside_down(v):
    at = 7 - lax.broadcasted_iota(jnp.int32, (8, v.shape[1]), 0)
    parts = [jnp.take_along_axis(v[i : i + 8], at, axis=0) for i in range(0, v.shape[0], 8)]
    return jnp.concatenate(parts[::-1], axis=0)


def x_kernel(even_ref, odd_ref, x_ref, a_ref, *refs):
    b_refs, (held, sems) = refs[:DEEP], refs[DEEP:]
    half = x_ref.shape[0] // 2
    me = lax.axis_index("deep")
    step, steps, slots = pl.program_id(0), pl.num_programs(0), held.shape[0]
    across = x_ref.shape[2] // 128

    def load(i):
        y, z = pl.multiple_of(i // across * 8, 8), pl.multiple_of(i % across * 128, 128)
        slot = lax.rem(i, slots)
        return pltpu.make_async_copy(x_ref.at[:, pl.ds(y, 8), pl.ds(z, 128)], held.at[slot], sems.at[slot])

    @pl.when(step == 0)
    def _():
        for i in range(slots):
            load(i).start()

    load(step).wait()
    even = even_ref[...].reshape(half, half)
    odd = jnp.concatenate([odd_ref[h, me ^ k] for h in range(2) for k in range(DEEP)], axis=0)
    a_rows = a_ref.reshape(half // 2 * 8, 128)
    b_rows = [b.reshape(NORTH * 8, 128) for b in b_refs]
    rows = held.reshape(slots * half * 2 * 8, 128)
    base = lax.rem(step, slots) * half * 2 * 8

    for y in range(0, 8, 2):
        near, far = (
            jnp.concatenate(
                [rows[pl.ds(base + first * half * 8 + y + j, half, stride=8), :] for j in range(2)], axis=1
            )
            for first in range(2)
        )
        far = upside_down(far)
        e = product(even, near + far)
        o = product(odd, near - far)
        for j in range(2):
            lanes = slice(j * 128, j * 128 + 128)
            a_rows[pl.ds(y + j, half // 2, stride=8), :] = e[:, lanes]
            for k in range(DEEP):
                b_rows[k][pl.ds(y + j, NORTH, stride=8), :] = o[k * NORTH : (k + 1) * NORTH, lanes]

    @pl.when(step + slots < steps)
    def _():
        load(step + slots).start()


def x_stage(source):
    nx, ny, nz = source.shape
    modes = nx // 2
    block = modes // NORTH
    near = np.arange(nx // 2)
    even = np.stack(halves(sines(near, np.arange(0, modes, 2), nx).T))
    odd_modes = (block * np.arange(NORTH)[None, :] + 2 * np.arange(DEEP)[:, None] + 1).reshape(-1)
    odd = np.stack(halves(sines(near, odd_modes, nx).T)).reshape(2, DEEP, NORTH, -1)
    across = nz // 128
    steps = ny // 8 * across
    b_shape = jax.ShapeDtypeStruct((NORTH, ny, nz), F32)
    b_spec = pl.BlockSpec((NORTH, 8, 128), lambda i: (0, i // across, i % across))
    return pl.pallas_call(
        x_kernel,
        grid=(steps,),
        in_specs=[vmem(), vmem(), pl.BlockSpec(memory_space=pl.ANY)],
        out_specs=[pl.BlockSpec((modes // 2, 8, 128), lambda i: (0, i // across, i % across))] + [b_spec] * DEEP,
        out_shape=[jax.ShapeDtypeStruct((modes // 2, ny, nz), F32)] + [b_shape] * DEEP,
        scratch_shapes=[pltpu.VMEM((4, nx, 8, 128), F32), pltpu.SemaphoreType.DMA((4,))],
        cost_estimate=cost(6 * nx * modes * ny * nz // 2, 6 * nx * ny * nz),
        name="x_stage",
    )(jnp.asarray(even), jnp.asarray(odd), source)


def y_table(ny):
    return jnp.asarray(wide(sines(np.arange(ny), np.arange(ny // 2), ny).T).reshape(DEEP, ny // 2 // DEEP, -1))


def ya_kernel(first, table_ref, v_ref, *refs):
    outs, (held, sems) = refs[:DEEP], refs[DEEP:]
    me, j = lax.axis_index("deep"), pl.program_id(0)

    def load(i):
        return pltpu.make_async_copy(v_ref.at[:, first + i], held.at[i], sems.at[i])

    @pl.when(j == 0)
    def _():
        for i in range(held.shape[0]):
            load(i).start()

    load(j).wait()
    table = jnp.concatenate([table_ref[me ^ k] for k in range(DEEP)], axis=0)
    n, y, z = held.shape[1:]
    m, block = table.shape[0] // DEEP, 256
    for i in range(z // block):
        at = slice(i * block, (i + 1) * block)
        r = dot(table, tall(held[j, :, :, at].reshape(n * y, block)))
        for k in range(DEEP):
            outs[k][0, :, at] = r[k * m : (k + 1) * m]


def ya_stage(table, v, first, js):
    n, _, y, nz = v.shape
    m = table.shape[1]
    return pl.pallas_call(
        functools.partial(ya_kernel, first),
        grid=(js,),
        in_specs=[vmem(), pl.BlockSpec(memory_space=pltpu.HBM)],
        out_specs=[pl.BlockSpec((1, m, nz), lambda j: (j, 0, 0))] * DEEP,
        out_shape=[jax.ShapeDtypeStruct((js, m, nz), F32)] * DEEP,
        scratch_shapes=[pltpu.VMEM((js, n, y, nz), F32), pltpu.SemaphoreType.DMA((js,))],
        cost_estimate=cost(6 * n * y * m * DEEP * js * nz, 6 * n * js * y * nz),
        compiler_params=LIMIT,
        name="ya_stage",
    )(table, v)


def backwards(v):
    lanes = v.shape[-1] // 128
    at = 127 - lax.broadcasted_iota(jnp.int32, (v.shape[0], 128), 1)
    parts = [v[:, i * 128 : (i + 1) * 128] for i in range(lanes)]
    return jnp.concatenate([jnp.take_along_axis(p, at, axis=1) for p in parts[::-1]], axis=1)


def shuffled(even, odd):
    lane = lax.broadcasted_iota(jnp.int32, (even.shape[0], 128), 1)
    parts = []
    for i in range(even.shape[1] // 128):
        e, o = even[:, i * 128 : (i + 1) * 128], odd[:, i * 128 : (i + 1) * 128]
        for at in (lane // 2, lane // 2 + 64):
            e_at, o_at = jnp.take_along_axis(e, at, axis=1), jnp.take_along_axis(o, at, axis=1)
            parts.append(jnp.where(lane % 2 == 0, e_at, o_at))
    return jnp.concatenate(parts, axis=1)


def z_halves(near, far, table):
    far = backwards(far)
    count = near.shape[0]
    both = []
    for parity, v in enumerate((near + far, near - far)):
        high, low = split(v)
        r = dot(jnp.concatenate([high, low], axis=0), table[parity, 0])
        both.append(r[:count] + r[count:] + dot(high, table[parity, 1]))
    return both


def zb_rows(table_ref, near, far, before, o_ref):
    n, y, z = near.shape
    both = z_halves(near.reshape(n * y, z), far.reshape(n * y, z), table_ref)
    for i in range(o_ref.shape[1]):
        for p in range(2):
            r = both[p][:, i * 128 : (i + 1) * 128].reshape(n, y, 128)
            lanes = slice(p * 128, p * 128 + 128)
            o_ref[:, i, :, lanes] = r if before is None else r + before[:, i, :, lanes]


def zb1_kernel(table_ref, near_ref, far_ref, o_ref):
    zb_rows(table_ref, near_ref[...], far_ref[...], None, o_ref)


def zb2_kernel(table_ref, before_ref, near_ref, far_ref, o_ref, near, far, sems):
    step = pl.program_id(0)
    rows = o_ref.shape[0]

    def loads(i):
        return [
            pltpu.make_async_copy(ref.at[pl.ds(i * rows, rows)], held.at[pl.ds(i * rows, rows)], sems.at[i, k])
            for k, (ref, held) in enumerate(((near_ref, near), (far_ref, far)))
        ]

    @pl.when(step == 0)
    def _():
        for i in range(near.shape[0] // rows):
            for copy in loads(i):
                copy.start()

    for copy in loads(step):
        copy.wait()
    at = pl.ds(step * rows, rows)
    zb_rows(table_ref, near[at], far[at], before_ref, o_ref)


def zb_stage(table, near, far, before=None):
    n, y, z = near.shape
    modes, rows = 2 * table.shape[3], 8
    spec = pl.BlockSpec((rows, y, z), lambda i: (i, 0, 0))
    wide_spec = pl.BlockSpec((rows, modes // 256, y, 256), lambda i: (i, 0, 0, 0))
    hbm = pl.BlockSpec(memory_space=pltpu.HBM)
    first = before is None
    shape = (n, modes // 256, y, 256)
    return pl.pallas_call(
        zb1_kernel if first else zb2_kernel,
        grid=(n // rows,),
        in_specs=[vmem(), spec, spec] if first else [vmem(), wide_spec, hbm, hbm],
        out_specs=wide_spec,
        out_shape=jax.ShapeDtypeStruct(shape, F32) if first else pltpu.HBM(shape, F32),
        scratch_shapes=[]
        if first
        else [pltpu.VMEM((n, y, z), F32)] * 2 + [pltpu.SemaphoreType.DMA((n // rows, 2))],
        cost_estimate=cost(6 * n * y * z * modes, 8 * n * y * (z + modes)),
        compiler_params=LIMIT,
        name="zb_stage",
    )(*((table, near, far) if first else (table, before, near, far)))


def za_kernel(first, sx_ref, t0_ref, t1_ref, sy_ref, sz_ref, p0, p1, p2, p3, *rest):
    o_ref = rest[-1]
    m, z = p0.shape[1], p0.shape[2]
    even0, odd0 = z_halves(p0[...].reshape(m, z), p3[...].reshape(m, z), t0_ref)
    even1, odd1 = z_halves(p1[...].reshape(m, z), p2[...].reshape(m, z), t1_ref)
    total = shuffled(even0 + even1, odd0 + odd1)
    yz = jnp.concatenate([sy_ref[lax.axis_index("deep")]] * (o_ref.shape[3] // 128), axis=1) + sz_ref[...]
    mode = (lax.axis_index("north") * DEEP + first + pl.program_id(0)) * 2
    o_ref[0, 0] = total * lax.rsqrt(sx_ref[mode] + yz)


def za_stage(sx, tables, sy, sz, pieces, first, *whole):
    js, m, z = pieces[0].shape
    modes = 2 * tables[0].shape[3]
    spec = pl.BlockSpec((1, m, z), lambda j: (j, 0, 0))
    return pl.pallas_call(
        functools.partial(za_kernel, first),
        grid=(js,),
        in_specs=[pl.BlockSpec(memory_space=pltpu.SMEM)]
        + [vmem()] * 4
        + [spec] * DEEP
        + [pl.BlockSpec(memory_space=pl.ANY)] * len(whole),
        out_specs=pl.BlockSpec((1, 1, m, modes), lambda j: (first + j, 0, 0, 0)),
        out_shape=jax.ShapeDtypeStruct((DEEP, 2, m, modes), F32),
        input_output_aliases={5 + DEEP: 0} if whole else {},
        cost_estimate=cost(6 * js * m * z * 2 * modes, 4 * js * m * z * DEEP + 8 * z * modes),
        compiler_params=LIMIT,
        name="za_stage",
    )(sx, *tables, sy, sz, *pieces, *whole)


def yb_kernel(sx_ref, table_ref, sy_ref, sz_ref, v_ref, *outs):
    me = lax.axis_index("deep")
    n, blocks, y, block = v_ref.shape
    table = jnp.concatenate([table_ref[me ^ k] for k in range(DEEP)], axis=0)
    m = table.shape[0] // DEEP
    sx = sx_ref[lax.axis_index("north") * 2 * DEEP + 2 * me + 1]
    for b in range(blocks):
        r = dot(table, tall(v_ref[:, b].reshape(n * y, block)))
        lanes = slice(b * block, (b + 1) * block)
        for k in range(DEEP):
            symbol = sx + jnp.concatenate([sy_ref[me ^ k]] * (block // 128), axis=1) + sz_ref[:, lanes]
            rows = slice(k * m, (k + 1) * m)
            outs[k][:, lanes] = shuffled(r[rows, : block // 2], r[rows, block // 2 :]) * lax.rsqrt(symbol)


def yb_stage(sx, table, sy, sz, v, part, parts):
    n, blocks, y, block = v.shape
    m = table.shape[1]
    blocks //= parts
    modes = blocks * block
    return pl.pallas_call(
        yb_kernel,
        grid=(1,),
        in_specs=[
            pl.BlockSpec(memory_space=pltpu.SMEM),
            vmem(),
            vmem(),
            pl.BlockSpec((1, modes), lambda i: (0, part)),
            pl.BlockSpec((n, blocks, y, block), lambda i: (0, part, 0, 0)),
        ],
        out_specs=[pl.BlockSpec((m, modes), lambda i: (0, 0))] * DEEP,
        out_shape=[jax.ShapeDtypeStruct((m, modes), F32)] * DEEP,
        cost_estimate=cost(6 * n * y * m * DEEP * modes, 6 * n * y * modes),
        compiler_params=LIMIT,
        name="yb_stage",
    )(sx, table, sy, sz, v)


def join_kernel(whole_ref, *refs):
    pieces, (o_ref, sems) = refs[:-2], refs[-2:]
    me = lax.axis_index("deep")
    copies = []
    for i, piece in enumerate(pieces):
        part, k = divmod(i, DEEP)
        modes = piece.shape[1]
        place = o_ref.at[me ^ k, 1, :, pl.ds(part * modes, modes)]
        copies.append(pltpu.make_async_copy(piece, place, sems.at[i]))
    for copy in copies:
        copy.start()
    for copy in copies:
        copy.wait()


def join_stage(whole, pieces):
    return pl.pallas_call(
        join_kernel,
        in_specs=[pl.BlockSpec(memory_space=pl.ANY)] + [vmem()] * len(pieces),
        out_specs=pl.BlockSpec(memory_space=pl.ANY),
        out_shape=jax.ShapeDtypeStruct(whole.shape, F32),
        scratch_shapes=[pltpu.SemaphoreType.DMA((len(pieces),))],
        input_output_aliases={0: 0},
        cost_estimate=cost(1, 8 * pieces[0].size * len(pieces)),
        compiler_params=LIMIT,
        name="join_stage",
    )(whole, *pieces)


def z_table(count, pair):
    stretch = lax.axis_index("deep") ^ pair
    point = (stretch * (count // DEEP) + jnp.arange(count // DEEP))[None, :, None]
    mode = (2 * jnp.arange(count // 4) + jnp.arange(2)[:, None])[:, None, :]
    turn = (point + 1) * (mode + 1) % (2 * count + 2)
    table = jnp.sin(np.float32(np.pi / (count + 1)) * turn.astype(F32)) * np.float32((2.0 / (count + 1)) ** 0.5)
    high = lax.reduce_precision(table, 8, 7)
    return jnp.stack([high, table - high], axis=1).astype(BF16)


def deep_exchange(pieces):
    got = [pieces[0]] + [None] * (DEEP - 1)
    for k in (1, 3, 2):
        got[k] = lax.ppermute(pieces[k], "deep", [(s, s ^ k) for s in range(DEEP)])
    return got


def north_exchange(v):
    return lax.all_to_all(v, "north", split_axis=0, concat_axis=0, tiled=True)


def on_device(source, symbol_x, symbol_y, symbol_z):
    ny, nz = source.shape[1] * NORTH, source.shape[2] * DEEP
    a, *b = x_stage(source)
    b = deep_exchange(b)
    a = north_exchange(a.reshape(NORTH, -1, *a.shape[1:]))
    tz = [z_table(nz, q) for q in range(2)]
    ty = y_table(ny)
    sy = jnp.broadcast_to(symbol_y[: ny // 2, None], (ny // 2, 128)).reshape(DEEP, -1, 128)
    sz = symbol_z[None, : nz // 2]
    part = zb_stage(tz[0], b[0], b[3])
    part = zb_stage(tz[1], b[1], b[2], part)
    b = north_exchange(part)
    a = [deep_exchange(ya_stage(ty, a, 2 * h, 2)) for h in range(2)]
    whole = za_stage(symbol_x, tz, sy, sz, a[0], 0)
    parts = []
    for part in range(2):
        piece = yb_stage(symbol_x, ty, sy, sz, b, part, 2)
        parts += deep_exchange(piece)
    whole = za_stage(symbol_x, tz, sy, sz, a[1], 2, whole)
    whole = join_stage(whole, parts)
    return whole.reshape(-1, *whole.shape[2:])


def solution(mesh):
    in_specs = (P(None, "north", "deep"), P(), P(), P())
    out_specs = P("north", "deep", None)
    return jax.shard_map(on_device, mesh=mesh, in_specs=in_specs, out_specs=out_specs, check_vma=False)
```
